256 devices in a mesh: dp: 4 (over x), expert: 32 (over y, z), tensor: 2 (over core).
Axes of the slice: x: 4, y: 4, z: 8, core: 2. Of those that a mesh axis runs over, the one named last changes fastest.
Arguments:
- tokens: bfloat16 [16384, 2560], P(('dp', 'expert')), may hold values from -6 to 6
- norm_gain: float32 [2560], replicated, may hold values from 0.5 to 1.5
- expert_ids: int32 [16384, 6], P(('dp', 'expert')), may hold values from 0 to 31, all different within a row; in each aligned block of 128 rows (0 to 127, 128 to 255, ...) at most 48 rows name the same one
- route_weights: int32 [16384, 6], P(('dp', 'expert')), may hold values from 1 to 64
- w_gate: bfloat16 [32, 2560, 768], P('expert', None, 'tensor'), may hold values from -0.125 to 0.125
- w_up: bfloat16 [32, 2560, 768], P('expert', None, 'tensor'), may hold values from -0.125 to 0.125
- w_down: bfloat16 [32, 768, 2560], P('expert', 'tensor'), may hold values from -0.21875 to 0.21875
- shared_gate: bfloat16 [2560, 2048], P(None, ('dp', 'tensor')), may hold values from -0.125 to 0.125
- shared_up: bfloat16 [2560, 2048], P(None, ('dp', 'tensor')), may hold values from -0.125 to 0.125
- shared_down: bfloat16 [2048, 2560], P(('dp', 'tensor')), may hold values from -0.125 to 0.125
Outputs:
- mixed: bfloat16 [16384, 2560], P(('dp', 'expert'), 'tensor')
The draws below stay inside these ranges and needn't reach their ends.
Inputs may be any that keep to these rules, and one draw needn't show every extreme that they name: `expert_ids`: each row names 6 different experts. In each aligned block of 128 rows (the rows of one index of dp+expert) no expert is named by more than 48 rows, a bound that some blocks reach.
All inputs are finite; a program needn't handle non-finite values.
Results may differ from the reference program's by a relative error of at most 0.011.
Values may be sent and summed in bfloat16 or wider, within the bound.
No kernel may reach another device: no remote copies, remote signals or barrier semaphores. Data moves between devices by JAX's collectives and lax.ppermute only.
A program may use at most 128 MiB of HBM per device.

```python
import math
import jax
import jax.numpy as jnp
import numpy as np
from jax import lax

D = 2560
FF = 768
SFF = 2048
EXPERTS = 32
TOP = 6
TOK_DEV = 128
CAP = 48
TOKENS = 16384


def place_ends(values, own_key, low, largest):
    spot = [jax.random.randint(jax.random.fold_in(own_key, axis), (), 0, length) for axis, length in enumerate(values.shape)]
    widest = values.shape.index(max(values.shape))
    next_to = spot[:widest] + [(spot[widest] + 1) % values.shape[widest]] + spot[widest + 1:]
    return values.at[tuple(spot)].set(low).at[tuple(next_to)].set(largest)


def shard_levels(rng, extent, split, low, largest):
    loudness = 1.0
    for dim, parts in split:
        draws = jax.random.uniform(jax.random.fold_in(jax.random.fold_in(rng, 6), dim), (parts,), jnp.float32, low / len(split), largest / len(split))
        loudness = loudness * jnp.repeat(jnp.exp(draws), extent[dim] // parts).reshape((-1,) + (1,) * (len(extent) - 1 - dim))
    return loudness


def deal_out(key, own, number, rows, number_of, top, reach, slope):
    ranking = jax.random.permutation(key, number_of)
    crowded, usual = portions_of(number_of, rows * top, reach, slope, True), portions_of(number_of, rows * top, reach, slope, False)
    places = jnp.arange(number_of)

    def named(tallies, offset_by):
        used = int((tallies > 0).sum())
        fixed = max(1, used // 4)
        shifted = fixed + (places - fixed + offset_by * (used - fixed)) % max(1, number_of - fixed)
        return jnp.zeros((number_of,), jnp.int32).at[ranking[jnp.where(places < fixed, places, shifted)]].set(jnp.asarray(tallies, jnp.int32))

    tallies = jnp.where(number % 4 == 0, named(crowded, number // 4), named(usual, number - number // 4 - 1))
    mixed = jax.random.permutation(jax.random.fold_in(own, 3), number_of)
    donor, taker = mixed[0:number_of // 2 * 2:2], mixed[1:number_of // 2 * 2:2]
    slack = jnp.minimum(tallies[donor] - 1, reach - tallies[taker]) // 2
    slack = jnp.where((donor == ranking[0]) | (taker == ranking[0]) | (tallies[taker] == 0), 0, jnp.maximum(slack, 0))
    shifted = jax.random.randint(jax.random.fold_in(own, 4), (number_of // 2,), 0, 1 << 20) % (slack + 1)
    tallies = tallies.at[donor].add(-shifted).at[taker].add(shifted)
    labels = jnp.searchsorted(jnp.cumsum(tallies), jnp.arange(rows * top), side="right").astype(jnp.int32)
    table = labels.reshape(top, rows).T
    table = table[jax.random.permutation(jax.random.fold_in(own, 1), rows)]
    offset_by = jax.random.randint(jax.random.fold_in(own, 2), (rows, 1), 0, top)
    return jnp.take_along_axis(table, (jnp.arange(top)[None, :] + offset_by) % top, axis=1)


def portions_of(count, total, limit, skew, full):
    portions = [(1 << 20) // math.isqrt(standing ** skew) + 1 for standing in range(1, count + 1)]
    largest = limit if full else min(limit, max(-(-total // count), total * portions[0] // sum(portions)))
    least = 1 if total - largest >= count - 1 else 0
    holding, rest = [largest] + [least] * (count - 1), total - largest - least * (count - 1)
    while rest > 0:
        movable = [i for i in range(1, count) if holding[i] < largest] or [i for i in range(1, count) if holding[i] < limit]
        pool, left = sum([portions[i] for i in movable]), rest
        for i in movable:
            extra = min(limit - holding[i], max(1, left * portions[i] // pool), rest)
            holding[i] = holding[i] + extra
            rest = rest - extra
    return np.array(holding)


def bell_draw(rng, dims, deviation, bound, cuts=(), kind=jnp.bfloat16):
    values = jax.random.normal(rng, dims, jnp.float32) * deviation
    if len(cuts) > 0:
        values = shard_levels(rng, dims, cuts, -0.22, 0.18) * values
    return jnp.clip(values, min=-bound, max=bound).astype(kind)


def setup_inputs(seed: int = 0) -> dict:
    keys = jax.random.split(jax.random.key(seed), 11)
    tokens = bell_draw(keys[0], (TOKENS, D), 1.0, 6.0, ((0, 128),))
    norm_gain = jnp.clip(1.0 + 0.1 * jax.random.normal(keys[1], (D,), jnp.float32), 0.5, 1.5)
    expert_ids_keys = jax.random.split(jax.random.fold_in(keys[2], 1), TOKENS // TOK_DEV)
    expert_ids_turns = jax.random.permutation(jax.random.fold_in(keys[2], 3), TOKENS // TOK_DEV)
    expert_ids = jax.vmap(lambda own, number: deal_out(jax.random.fold_in(keys[2], 2), own, number, TOK_DEV, EXPERTS, TOP, CAP, 2))(expert_ids_keys, expert_ids_turns).reshape((TOKENS, TOP))
    route_weights = place_ends(jax.random.randint(keys[3], (TOKENS, TOP), 1, 65), jax.random.fold_in(keys[3], 1), 1, 64).astype(jnp.int32)
    w_gate = bell_draw(keys[4], (EXPERTS, D, FF), D ** -0.5, 0.125, ((0, 32), (2, 2)))
    w_up = bell_draw(keys[5], (EXPERTS, D, FF), D ** -0.5, 0.125, ((0, 32), (2, 2)))
    w_down = bell_draw(keys[6], (EXPERTS, FF, D), FF ** -0.5, 0.21875, ((0, 32), (1, 2)))
    shared_gate = bell_draw(keys[7], (D, SFF), D ** -0.5, 0.125, ((1, 8),))
    shared_up = bell_draw(keys[8], (D, SFF), D ** -0.5, 0.125, ((1, 8),))
    shared_down = bell_draw(keys[9], (SFF, D), SFF ** -0.5, 0.125, ((0, 8),))
    return {"tokens": tokens, "norm_gain": norm_gain, "expert_ids": expert_ids, "route_weights": route_weights, "w_gate": w_gate, "w_up": w_up, "w_down": w_down, "shared_gate": shared_gate, "shared_up": shared_up, "shared_down": shared_down}


EPSILON = 1e-06

def normalize(tokens, norm_gain):
    values = tokens.astype(jnp.float32)
    inverse = lax.rsqrt(lax.optimization_barrier(jnp.mean(values * values, axis=1, keepdims=True)) + EPSILON)
    return (values * inverse * norm_gain.astype(jnp.float32)[None, :]).astype(jnp.bfloat16)

def reference(tokens, norm_gain, expert_ids, route_weights, w_gate, w_up, w_down, shared_gate, shared_up, shared_down):
    normed = normalize(tokens, norm_gain)
    groups = TOKENS // TOK_DEV
    pair_total = TOK_DEV * TOP
    local_ids = expert_ids.reshape(groups, pair_total).astype(jnp.int32)
    onehot = (local_ids[:, :, None] == jnp.arange(EXPERTS, dtype=jnp.int32)[None, None, :]).astype(jnp.int32)
    earlier = jnp.cumsum(onehot, axis=1) - onehot
    slot_index = lax.optimization_barrier(jnp.sum(earlier * onehot, axis=2)).astype(jnp.int32)
    position = (local_ids * CAP + slot_index).astype(jnp.int32)
    group_index = jnp.broadcast_to(jnp.arange(groups, dtype=jnp.int32)[:, None], (groups, pair_total)).astype(jnp.int32)
    pair_token = (group_index * TOK_DEV + jnp.arange(pair_total, dtype=jnp.int32)[None, :] // TOP).astype(jnp.int32)
    filler = jnp.full((groups, EXPERTS * CAP), -1, jnp.int32).at[group_index, position].set(pair_token)
    pair_scale = route_weights.astype(jnp.float32).reshape(groups, pair_total) / 64.0
    slot_scale = jnp.zeros((groups, EXPERTS * CAP), jnp.float32).at[group_index, position].set(pair_scale)
    filler = filler.reshape(groups, EXPERTS, CAP).transpose(1, 0, 2).reshape(EXPERTS, groups * CAP)
    slot_scale = slot_scale.reshape(groups, EXPERTS, CAP).transpose(1, 0, 2).reshape(EXPERTS, groups * CAP)

    def expert_step(totals, inputs):
        owner_rows, owner_scale, gate_weight, up_weight, down_weight = inputs
        valid = owner_rows >= 0
        safe_rows = jnp.maximum(owner_rows, 0).astype(jnp.int32)
        picked = jnp.where(valid[:, None], normed[safe_rows], jnp.zeros((), jnp.bfloat16))
        gate_value = jnp.dot(picked, gate_weight, preferred_element_type=jnp.float32)
        up_value = jnp.dot(picked, up_weight, preferred_element_type=jnp.float32)
        hidden = (jax.nn.silu(gate_value) * up_value).astype(jnp.bfloat16)
        result = jnp.dot(hidden, down_weight, preferred_element_type=jnp.float32).astype(jnp.bfloat16)
        update = result.astype(jnp.float32) * owner_scale[:, None]
        update = jnp.where(valid[:, None], update, jnp.zeros((), jnp.float32))
        return (totals.at[safe_rows].add(update), None)
    routed, unused = lax.scan(expert_step, jnp.zeros((TOKENS, D), jnp.float32), (filler, slot_scale, w_gate, w_up, w_down))
    shared_gate_value = jnp.dot(normed, shared_gate, preferred_element_type=jnp.float32)
    shared_up_value = jnp.dot(normed, shared_up, preferred_element_type=jnp.float32)
    shared_hidden = (jax.nn.silu(shared_gate_value) * shared_up_value).astype(jnp.bfloat16)
    shared_out = jnp.dot(shared_hidden, shared_down, preferred_element_type=jnp.float32)
    return (shared_out + routed).astype(jnp.bfloat16)
```

```python
import functools

import jax
import jax.numpy as jnp
from jax import lax
from jax.experimental import pallas as pl
from jax.experimental.pallas import tpu as pltpu
from jax.sharding import Mesh
from jax.sharding import PartitionSpec as P

D = 2560
HALF = 1280
EXPERTS = 32
TOP = 6
CAP = 48
ROWS = 128
NY = 4
NZ = 8
EXT = HALF + 128
EPSILON = 1e-06
BF = jnp.bfloat16
F32 = jnp.float32

GROUPS = ((0, -1, 1), (-2, 2), (-4, -3, 3))
SHIFTS = (0, 1, -1, 2)


VMEM = pl.BlockSpec(memory_space=pltpu.VMEM)
HBM = pl.BlockSpec(memory_space=pl.ANY)
META = pl.BlockSpec((ROWS, 128), lambda i: (0, HALF // 128))


def call(body, outs, in_specs, args, name, flops=0, scratch=()):
    return pl.pallas_call(
        body,
        grid=(1,),
        out_shape=[jax.ShapeDtypeStruct(s, d) for s, d in outs],
        in_specs=in_specs,
        out_specs=[VMEM] * len(outs),
        scratch_shapes=list(scratch),
        compiler_params=pltpu.CompilerParams(vmem_limit_bytes=60 * 2**20),
        cost_estimate=pl.CostEstimate(flops=flops, bytes_accessed=1 << 20, transcendentals=0),
        name=name,
    )(*args)


def dot(a, b):
    return jnp.dot(a, b, preferred_element_type=F32)


def prep_body(tokens, gain, ids, weights, normed, ext):
    values = tokens[...].astype(F32)
    inverse = lax.rsqrt(jnp.mean(values * values, axis=1, keepdims=True) + EPSILON)
    result = (values * inverse * gain[...]).astype(BF)
    normed[...] = result
    rank = lax.axis_index("tensor")
    ext[:, :HALF] = jnp.where(rank == 0, result[:, :HALF], result[:, HALF:])
    lanes = lax.broadcasted_iota(jnp.int32, (ROWS, 128), 1)
    rows = lax.broadcasted_iota(jnp.int32, (ROWS, 128), 0)
    named = jnp.zeros((ROWS, 128), F32)
    scale = jnp.zeros((ROWS, 128), F32)
    for k in range(TOP):
        same = lanes == ids[:, k : k + 1]
        named = jnp.where(same, 1.0, named)
        same_w = lanes == ids[:, k : k + 1] + EXPERTS
        scale = jnp.where(same_w, weights[:, k : k + 1].astype(F32) * (1.0 / 64.0), scale)
    lower = jnp.where(lanes <= rows, 1.0, 0.0).astype(BF)
    counted = dot(lower, named.astype(BF))
    slots = jnp.where(named > 0.0, counted - 1.0, -1.0)
    ext[:, HALF:] = jnp.where(lanes < EXPERTS, slots, scale).astype(BF)


def prep(tokens, norm_gain, ids, weights):
    return call(
        prep_body,
        [((ROWS, D), BF), ((ROWS, EXT), BF)],
        [VMEM] * 4,
        (tokens, norm_gain.reshape(1, D), ids, weights),
        "prep",
        flops=40_000_000,
    )


def expert_of(shift):
    return ((lax.axis_index("y") + NY + shift) % NY) * NZ + lax.axis_index("z")


def gather_body(n, *refs):
    exts, outs = refs[:n], refs[n:]
    for i in range(n):
        meta = exts[i][:, HALF:].astype(F32).T
        which = lax.broadcasted_iota(jnp.int32, (128, ROWS), 0)
        slot = lax.broadcasted_iota(jnp.int32, (CAP, ROWS), 0).astype(F32)
        picks = []
        for shift in SHIFTS:
            row = jnp.sum(jnp.where(which == expert_of(shift), meta, 0.0), axis=0, keepdims=True)
            picks.append(jnp.where(slot == row, 1.0, 0.0))
        pick = jnp.concatenate(picks, axis=0).astype(BF)
        rows = dot(pick, exts[i][:, :HALF]).astype(BF)
        for j in range(4):
            outs[j][i * CAP : (i + 1) * CAP, :] = rows[j * CAP : (j + 1) * CAP, :]


def gather(exts):
    n = len(exts)
    return call(
        functools.partial(gather_body, n),
        [((n * CAP, HALF), BF)] * 4,
        [VMEM] * n,
        exts,
        "gather",
        flops=63_000_000 * n,
    )


def combine_block(meta_ref, row_refs, i):
    meta = meta_ref[...].astype(F32)
    lanes = lax.broadcasted_iota(jnp.int32, (ROWS, 128), 1)
    place = lax.broadcasted_iota(jnp.int32, (ROWS, 4 * CAP), 1).astype(F32)
    mix = jnp.zeros((ROWS, 4 * CAP), F32)
    for j, shift in enumerate(SHIFTS):
        e = expert_of(shift)
        slot = jnp.sum(jnp.where(lanes == e, meta, 0.0), axis=1, keepdims=True)
        scale = jnp.sum(jnp.where(lanes == e + EXPERTS, meta, 0.0), axis=1, keepdims=True)
        hit = (place == slot + float(j * CAP)) & (slot >= 0.0)
        mix = jnp.where(hit, scale, mix)
    rows = jnp.concatenate([r[i * CAP : (i + 1) * CAP, :] for r in row_refs], axis=0)
    return dot(mix.astype(BF), rows)


def combine_body(places, accs, *refs):
    metas, refs = refs[: len(places)], refs[len(places) :]
    rows, refs = refs[:4], refs[4:]
    taken, outs = refs[: sum(accs)], refs[sum(accs) :]
    used = 0
    for b, (i, has) in enumerate(zip(places, accs)):
        value = combine_block(metas[b], rows, i)
        if has:
            value = value + taken[used][...].astype(F32)
            used += 1
        outs[b][...] = value.astype(BF)


def combine(places, exts, rows, accs):
    present = [a is not None for a in accs]
    return call(
        functools.partial(combine_body, tuple(places), tuple(present)),
        [((ROWS, HALF), BF)] * len(places),
        [META] * len(places) + [VMEM] * (4 + sum(present)),
        [*exts, *rows, *[a for a in accs if a is not None]],
        "combine",
        flops=63_000_000 * len(places),
    )


def final_body(place, meta, *refs):
    rows, refs = refs[:4], refs[4:]
    shared, parts, out = refs[0], refs[1:-1], refs[-1]
    value = combine_block(meta, rows, place) + shared[...]
    for part in parts:
        value = value + part[...].astype(F32)
    out[...] = value.astype(BF)


def ffn_body(n, own, other, wg0, wu0, wg1, wu1, wd0, wd1, *refs):
    outs = refs[:4]
    bg0, bu0, bg1, bu1, bd0, bd1, total, sems = refs[4:]
    rank = lax.axis_index("tensor")
    mine = pl.ds(pl.multiple_of(rank * HALF, HALF), HALF)
    theirs = pl.ds(pl.multiple_of((1 - rank) * HALF, HALF), HALF)
    copies = []
    for k, (src, dst) in enumerate(
        ((wg0, bg0), (wu0, bu0), (wd0.at[:, mine], bd0), (wg1, bg1), (wu1, bu1), (wd1, bd1))
    ):
        c = pltpu.make_async_copy(src, dst, sems.at[k])
        c.start()
        copies.append(c)
    left, right = own[...], other[...]
    for half, (bg, bu, bd) in enumerate(((bg0, bu0, bd0), (bg1, bu1, bd1))):
        copies[3 * half].wait()
        gate = dot(left, bg[mine, :]) + dot(right, bg[theirs, :])
        copies[3 * half + 1].wait()
        up = dot(left, bu[mine, :]) + dot(right, bu[theirs, :])
        hidden = (gate / (1.0 + jnp.exp(-gate)) * up).astype(BF)
        copies[3 * half + 2].wait()
        part = dot(hidden, bd[...])
        if half == 0:
            total[...] = part
        else:
            result = (total[...] + part).astype(BF)
            for j in range(4):
                outs[j][...] = result[j * n * CAP : (j + 1) * n * CAP, :]


def ffn(n, own, other, weights):
    rows = 4 * n * CAP
    wide = pltpu.VMEM((D, 384), BF)
    down = pltpu.VMEM((384, HALF), BF)
    return call(
        functools.partial(ffn_body, n),
        [((n * CAP, HALF), BF)] * 4,
        [VMEM, VMEM] + [HBM] * 6,
        (own, other, *weights),
        "ffn",
        flops=2 * rows * 768 * (2 * D + HALF),
        scratch=(wide, wide, wide, wide, down, down, pltpu.VMEM((rows, HALF), F32), pltpu.SemaphoreType.DMA((6,))),
    )


def shared_body(b0, b1, b2, b3, wg, wu, wd, keep, send):
    rank = lax.axis_index("tensor")
    for i, block in enumerate((b0, b1, b2, b3)):
        value = block[...]
        gate = dot(value, wg[...])
        up = dot(value, wu[...])
        hidden = (gate / (1.0 + jnp.exp(-gate)) * up).astype(BF)
        part = dot(hidden, wd[...])
        low, high = part[:, :HALF], part[:, HALF:]
        at = slice(i * ROWS, (i + 1) * ROWS)
        keep[at, :] = jnp.where(rank == 0, low, high)
        send[at, :] = jnp.where(rank == 0, high, low).astype(BF)


def shared(blocks, wg, wu, wd):
    return call(
        shared_body,
        [((4 * ROWS, HALF), F32), ((4 * ROWS, HALF), BF)],
        [VMEM] * 7,
        (*blocks, wg, wu, wd),
        "shared",
        flops=2 * 4 * ROWS * 256 * 3 * D,
    )


def split_body(keep, got, own, *outs):
    own[...] = keep[:ROWS, :] + got[:ROWS, :].astype(F32)
    for i in range(3):
        at = slice((i + 1) * ROWS, (i + 2) * ROWS)
        outs[i][...] = (keep[at, :] + got[at, :].astype(F32)).astype(BF)


def move(value, axis, shift):
    count = lax.axis_size(axis)
    return lax.ppermute(value, axis, [(i, (i + shift) % count) for i in range(count)])


def on_device(
    tokens,
    norm_gain,
    expert_ids,
    route_weights,
    w_gate,
    w_up,
    w_down,
    shared_gate,
    shared_up,
    shared_down,
):
    rank = lax.axis_index("tensor")
    w_gate, w_up, w_down = w_gate[0], w_up[0], w_down[0]
    normed, ext = prep(tokens, norm_gain, expert_ids, route_weights)

    blocks = {0: ext}
    for k in range(1, 5):
        blocks[-k] = move(blocks[1 - k], "z", 1)
        if k < 4:
            blocks[k] = move(blocks[k - 1], "z", -1)

    their_gate = move(w_gate, "tensor", 1)
    their_up = move(w_up, "tensor", 1)
    their_down = move(lax.dynamic_slice_in_dim(w_down, (1 - rank) * HALF, HALF, 1), "tensor", 1)
    weights = (w_gate, w_up, their_gate, their_up, w_down, their_down)

    results = []
    for group in GROUPS:
        n = len(group)
        out = gather([blocks[b] for b in group])
        arrived = [out[0]] + [move(out[j], "y", SHIFTS[j]) for j in (1, 2, 3)]
        own = jnp.concatenate(arrived, axis=0)
        other = move(own, "tensor", 1)
        results.append((n, own, other))
    back = []
    for n, own, other in reversed(results):
        out = ffn(n, own, other, weights)
        back.append([out[0]] + [move(out[j], "y", -SHIFTS[j]) for j in (1, 2, 3)])
    back = back[::-1]

    around = [normed] + [move(normed, "dp", s) for s in (1, -1, 2)]
    keep, send = shared(around, shared_gate, shared_up, shared_down)
    got = move(send, "tensor", 1)
    mine, *others = call(
        split_body,
        [((ROWS, HALF), F32)] + [((ROWS, HALF), BF)] * 3,
        [VMEM] * 2,
        (keep, got),
        "split",
        flops=2_000_000,
    )
    shared_parts = [move(o, "dp", -s) for o, s in zip(others, (1, -1, 2))]

    def stage(group, offsets, accs):
        places = [GROUPS[group].index(o) for o in offsets]
        return combine(places, [blocks[o] for o in offsets], back[group], accs)

    (far,) = stage(2, (-4,), (None,))
    down = move(far, "z", -1)
    at_minus, at_plus = stage(2, (-3, 3), (down, None))
    for k, group in ((3, 1), (2, 0)):
        down, up = move(at_minus, "z", -1), move(at_plus, "z", 1)
        at_minus, at_plus = stage(group, (1 - k, k - 1), (down, up))
    down, up = move(at_minus, "z", -1), move(at_plus, "z", 1)
    return call(
        functools.partial(final_body, GROUPS[0].index(0)),
        [((ROWS, HALF), BF)],
        [META] + [VMEM] * 10,
        (ext, *back[0], mine, *shared_parts, down, up),
        "final",
        flops=63_000_000,
    )[0]


def solution(mesh):
    fine = Mesh(mesh.devices.reshape(4, NY, NZ, 2), ("dp", "y", "z", "tensor"))
    expert = ("y", "z")
    token = ("dp", "y", "z")
    placed = (
        P(token, None),
        P(),
        P(token, None),
        P(token, None),
        P(expert, None, "tensor"),
        P(expert, None, "tensor"),
        P(expert, "tensor", None),
        P(None, ("dp", "tensor")),
        P(None, ("dp", "tensor")),
        P(("dp", "tensor"), None),
    )
    return jax.shard_map(
        on_device,
        mesh=fine,
        in_specs=placed,
        out_specs=P(token, "tensor"),
        check_vma=False,
    )
```
